32 devices in a mesh: row: 8 (over y, x, core), col: 4 (over z).
Axes of the slice: x: 2, y: 2, z: 4, core: 2. Of those that a mesh axis runs over, the one named last changes fastest.
Arguments:
- matrix: float32 [16384, 8192], P('row', 'col'), may hold values from -40 to 40
Outputs:
- upper: float32 [256, 8192], P('row', 'col')
- reduced: float32 [16384, 8192], P('row', 'col')
The draws below stay inside these ranges and needn't reach their ends.
All inputs are finite; a program needn't handle non-finite values.
Results may differ from the reference program's by a relative error of at most 0.0003.
Values sent between devices are 32-bit elements; how exact they have to be, the bound alone decides.
A program may use at most 128 MiB of HBM per device.

```python
import jax
import jax.numpy as jnp
from jax import lax

COLS = 8192
PANEL = 256
ROWS = 16384


def draw_matrix(key, part):
    base = jax.random.normal(jax.random.fold_in(key, 1), (ROWS, COLS), jnp.float32)
    return jnp.clip(base, -40.0, 40.0)


def setup_inputs(seed: int = 0) -> dict:
    key_list = jax.random.split(jax.random.key(seed), 2)
    return {
        "matrix": draw_matrix(jax.random.fold_in(key_list[1], 71), 0),
    }


def reference(matrix):
    panel = matrix[:, :PANEL]
    basis, factor = jnp.linalg.qr(panel)
    signs = jnp.sign(jnp.diagonal(factor))
    basis = basis * signs[None, :]
    upper = jnp.dot(basis.T.astype(jnp.float32), matrix.astype(jnp.float32), precision=lax.Precision.HIGHEST, preferred_element_type=jnp.float32)
    rest = matrix[:, PANEL:] - jnp.dot(basis.astype(jnp.float32), upper[:, PANEL:].astype(jnp.float32), precision=lax.Precision.HIGHEST, preferred_element_type=jnp.float32)
    scale = jnp.sqrt(jnp.float32(ROWS))
    reduced = jnp.concatenate([basis * scale, rest], axis=1)
    return (upper, reduced)
```

```python
import functools

import jax
import jax.numpy as jnp
from jax import lax
from jax.experimental import pallas as pl
from jax.experimental.pallas import tpu as pltpu
from jax.sharding import PartitionSpec as P

PANEL = 256
BLOCK = 32
CHUNK = 128
TILE = 512
MESH = pl.DeviceIdType.MESH
precise = lax.Precision.HIGHEST


def multiply(left, right, dims=((1,), (0,))):
    return lax.dot_general(
        left, right, (dims, ((), ())), precision=precise, preferred_element_type=jnp.float32
    )


def quick(left, right):
    return jnp.dot(left, right, preferred_element_type=jnp.float32)


def split(value):
    high = value.astype(jnp.bfloat16)
    return high, (value - high.astype(jnp.float32)).astype(jnp.bfloat16)


def factor(work_ref, inverse_ref):
    row_ids = lax.broadcasted_iota(jnp.int32, (PANEL, PANEL), 0)
    col_ids = lax.broadcasted_iota(jnp.int32, (PANEL, PANEL), 1)
    work_ref[:, PANEL:] = (row_ids == col_ids).astype(jnp.float32)

    def step(k, carry):
        first = pl.multiple_of(k * BLOCK, BLOCK)
        rows = work_ref[pl.ds(first, BLOCK), :]
        picks_row = lax.broadcasted_iota(jnp.int32, (PANEL, 128), 0)
        picks_col = lax.broadcasted_iota(jnp.int32, (PANEL, 128), 1)
        picks = ((picks_row == picks_col + first) & (picks_col < BLOCK)).astype(jnp.float32)
        left = multiply(rows[:, :PANEL], picks)
        row = lax.broadcasted_iota(jnp.int32, (BLOCK, 128), 0)
        col = lax.broadcasted_iota(jnp.int32, (BLOCK, 128), 1)
        right = (row == col).astype(jnp.float32)
        for j in range(BLOCK):
            pivot = left[j : j + 1, j : j + 1]
            inv = lax.rsqrt(pivot)
            inv = inv * (1.5 - 0.5 * pivot * inv * inv)
            left_row = left[j : j + 1, :] * inv
            right_row = right[j : j + 1, :] * inv
            column = jnp.where(row > j, left[:, j : j + 1] * inv, 0.0)
            left = left - column * left_row
            right = jnp.where(row == j, right_row, right - column * right_row)
        solved = multiply(right[:, :BLOCK], rows)
        work_ref[pl.ds(first, BLOCK), :] = solved
        change = multiply(solved[:, :PANEL], solved, ((0,), (0,)))
        below = lax.broadcasted_iota(jnp.int32, (PANEL, 2 * PANEL), 0) >= first + BLOCK
        whole = work_ref[...]
        work_ref[...] = jnp.where(below, whole - change, whole)
        return carry

    lax.fori_loop(0, PANEL // BLOCK, step, 0)
    inverse_ref[...] = work_ref[:, PANEL:]


def gather_kernel(
    row_n,
    col_n,
    matrix_ref,
    panel_ref,
    inverse_ref,
    total_ref,
    products_ref,
    held_ref,
    gram_ref,
    gram_in_ref,
    work_ref,
    sums_in_ref,
    load_sem,
    panel_sem,
    chunk_send,
    chunk_recv,
    gram_send,
    gram_recv,
    inv_send,
    inv_recv,
    rs_send,
    rs_recv,
    ag_send,
    ag_recv,
):
    r = lax.axis_index("row")
    z = lax.axis_index("col")
    rows, cols = held_ref.shape
    chunks = rows // CHUNK
    half = chunks // 2
    blocks = rows // PANEL
    per_block = PANEL // CHUNK
    levels = row_n.bit_length() - 1

    parity = lax.rem(r, 2)
    bits = []
    for s in range(levels):
        even = 1 << s
        odd = 1 if s == 0 else 1 << (levels - s)
        bits.append(even + parity * (odd - even))
    mine = [lax.rem(lax.div(r, bit), 2) for bit in bits]
    partner = [r + bit * (1 - 2 * own) for bit, own in zip(bits, mine)]

    panel_load = pltpu.make_async_copy(
        matrix_ref.at[:, pl.ds(0, PANEL)], panel_ref, panel_sem
    )

    @pl.when(z == 0)
    def _():
        panel_load.start()

    def load(i):
        span = pl.ds(pl.multiple_of(i * PANEL, PANEL), PANEL)
        return pltpu.make_async_copy(matrix_ref.at[span, :], held_ref.at[span, :], load_sem.at[i])

    for i in range(blocks):
        load(i).start()

    barrier = pltpu.get_barrier_semaphore()
    for other in partner:
        pl.semaphore_signal(
            barrier, inc=1, device_id={"row": other, "col": z}, device_id_type=MESH
        )
    for d in range(1, col_n):
        pl.semaphore_signal(
            barrier,
            inc=1,
            device_id={"row": r, "col": lax.rem(z + d, col_n)},
            device_id_type=MESH,
        )
    products_ref[...] = jnp.zeros_like(products_ref)
    pl.semaphore_wait(barrier, levels + col_n - 1)

    def send_chunk(i, to):
        span = pl.ds(pl.multiple_of(i * CHUNK, CHUNK), CHUNK)
        return pltpu.make_async_remote_copy(
            src_ref=panel_ref.at[span, :],
            dst_ref=panel_ref.at[span, :],
            send_sem=chunk_send.at[i],
            recv_sem=chunk_recv.at[i],
            device_id={"row": r, "col": to},
            device_id_type=MESH,
        )

    up = lax.rem(z + 1, col_n)
    down = lax.rem(z + col_n - 1, col_n)

    def add_block(i):
        load(i).wait()
        span = pl.ds(pl.multiple_of(i * PANEL, PANEL), PANEL)
        high, low = split(panel_ref[span, :].T)
        for c in range(0, cols, TILE):
            m_high, m_low = split(held_ref[span, pl.ds(c, TILE)])
            products_ref[:, pl.ds(c, TILE)] += (
                quick(high, m_high) + quick(high, m_low) + quick(low, m_high)
            )

    def send_inverse(d):
        return pltpu.make_async_remote_copy(
            src_ref=inverse_ref,
            dst_ref=inverse_ref,
            send_sem=inv_send.at[d - 1],
            recv_sem=inv_recv,
            device_id={"row": r, "col": lax.rem(z + d, col_n)},
            device_id_type=MESH,
        )

    @pl.when(z == 0)
    def _():
        panel_load.wait()
        for i in range(half):
            send_chunk(i, up).start()
            send_chunk(half + i, down).start()
        gram_ref[...] = jnp.zeros_like(gram_ref)

        def gram_block(i, carry):
            part = panel_ref[pl.ds(pl.multiple_of(i * PANEL, PANEL), PANEL), :]
            gram_ref[...] += multiply(part, part, ((0,), (0,)))
            return carry

        lax.fori_loop(0, blocks, gram_block, 0)
        for s in range(levels):
            copy = pltpu.make_async_remote_copy(
                src_ref=gram_ref,
                dst_ref=gram_in_ref.at[s],
                send_sem=gram_send.at[s],
                recv_sem=gram_recv.at[s],
                device_id={"row": partner[s], "col": z},
                device_id_type=MESH,
            )
            copy.start()

            def filler(i, carry):
                add_block(i)
                return carry

            lax.fori_loop(blocks * s // levels, blocks * (s + 1) // levels, filler, 0)
            copy.wait()
            gram_ref[...] += gram_in_ref[s]
        work_ref[:, :PANEL] = gram_ref[...]
        factor(work_ref, inverse_ref)
        for d in range(1, col_n):
            send_inverse(d).start()

    @pl.when(z > 0)
    def _():
        def slot(t, carry):
            one = t - z
            two = t - (col_n - z)

            @pl.when((one >= 0) & (one < half))
            def _():
                copy = send_chunk(one, up)
                copy.wait_recv()

                @pl.when(z < col_n - 1)
                def _():
                    copy.start()

            @pl.when((two >= 0) & (two < half))
            def _():
                copy = send_chunk(half + two, down)
                copy.wait_recv()

                @pl.when(z > 1)
                def _():
                    copy.start()

            @pl.when((one >= 0) & (one < half) & (lax.rem(one + per_block, per_block) == per_block - 1))
            def _():
                add_block(lax.div(one, per_block))

            @pl.when((two >= 0) & (two < half) & (lax.rem(two + per_block, per_block) == per_block - 1))
            def _():
                add_block(lax.div(half + two, per_block))

            return carry

        lax.fori_loop(1, half + col_n - 1, slot, 0)

    low = 0
    size = PANEL
    offset = 0
    spans = []
    for s in range(levels):
        size //= 2
        keep = pl.multiple_of(low + mine[s] * size, size)
        give = pl.multiple_of(low + (1 - mine[s]) * size, size)
        copy = pltpu.make_async_remote_copy(
            src_ref=products_ref.at[pl.ds(give, size), :],
            dst_ref=sums_in_ref.at[pl.ds(offset, size), :],
            send_sem=rs_send.at[s],
            recv_sem=rs_recv.at[s],
            device_id={"row": partner[s], "col": z},
            device_id_type=MESH,
        )
        copy.start()
        copy.wait()
        summed_ref = total_ref if s == levels - 1 else products_ref
        summed_ref[pl.ds(keep, size), :] = (
            products_ref[pl.ds(keep, size), :] + sums_in_ref[pl.ds(offset, size), :]
        )
        spans.append((keep, size))
        low = keep
        offset += size
    for s in reversed(range(levels)):
        keep, size = spans[s]
        span = pl.ds(keep, size)
        copy = pltpu.make_async_remote_copy(
            src_ref=total_ref.at[span, :],
            dst_ref=total_ref.at[span, :],
            send_sem=ag_send.at[s],
            recv_sem=ag_recv.at[s],
            device_id={"row": partner[s], "col": z},
            device_id_type=MESH,
        )
        copy.start()
        copy.wait()

    @pl.when(z == 0)
    def _():
        for d in range(1, col_n):
            send_inverse(d).wait_send()

    @pl.when(z > 0)
    def _():
        send_inverse(1).wait_recv()

    def drain(i, carry):
        @pl.when(z < col_n - 1)
        def _():
            send_chunk(i, up).wait_send()

        @pl.when(z != 1)
        def _():
            send_chunk(half + i, down).wait_send()

        return carry

    lax.fori_loop(0, half, drain, 0)


def project_kernel(
    total_rows, share_rows, matrix_ref, panel_ref, inverse_ref, products_ref,
    share_ref, reduced_ref, high_ref, low_ref,
):
    r = lax.axis_index("row")
    z = lax.axis_index("col")
    cols = matrix_ref.shape[1]

    @pl.when(pl.program_id(0) == 0)
    def _():
        for c in range(0, cols, TILE):
            upper = multiply(inverse_ref[...], products_ref[:, pl.ds(c, TILE)])
            high_ref[:, pl.ds(c, TILE)], low_ref[:, pl.ds(c, TILE)] = split(upper)
        mine = pl.ds(pl.multiple_of(r * share_rows, share_rows), share_rows)
        for c in range(0, cols, TILE):
            share_ref[:, pl.ds(c, TILE)] = multiply(
                inverse_ref[mine, :], products_ref[:, pl.ds(c, TILE)]
            )

    basis = multiply(panel_ref[...], inverse_ref[...], ((1,), (1,)))
    high, low = split(basis)
    for c in range(0, cols, TILE):
        u_high = high_ref[:, pl.ds(c, TILE)]
        reduced_ref[:, pl.ds(c, TILE)] = matrix_ref[:, pl.ds(c, TILE)] - (
            quick(high, u_high) + quick(high, low_ref[:, pl.ds(c, TILE)]) + quick(low, u_high)
        )

    @pl.when(z == 0)
    def _():
        reduced_ref[:, :PANEL] = basis * (total_rows**0.5)


def shards(matrix):
    row_n = lax.axis_size("row")
    col_n = lax.axis_size("col")
    rows, cols = matrix.shape
    levels = row_n.bit_length() - 1
    chunks = rows // CHUNK
    dma = pltpu.SemaphoreType.DMA
    vmem = pl.BlockSpec(memory_space=pltpu.VMEM)
    panel, inverse, products = pl.pallas_call(
        functools.partial(gather_kernel, row_n, col_n),
        out_shape=(
            jax.ShapeDtypeStruct((rows, PANEL), jnp.float32),
            jax.ShapeDtypeStruct((PANEL, PANEL), jnp.float32),
            jax.ShapeDtypeStruct((PANEL, cols), jnp.float32),
        ),
        in_specs=[pl.BlockSpec(memory_space=pl.ANY)],
        out_specs=(vmem, vmem, vmem),
        scratch_shapes=[
            pltpu.VMEM((PANEL, cols), jnp.float32),
            pltpu.VMEM((rows, cols), jnp.float32),
            pltpu.VMEM((PANEL, PANEL), jnp.float32),
            pltpu.VMEM((levels, PANEL, PANEL), jnp.float32),
            pltpu.VMEM((PANEL, 2 * PANEL), jnp.float32),
            pltpu.VMEM((PANEL, cols), jnp.float32),
            dma((rows // PANEL,)),
            dma,
            dma((chunks,)),
            dma((chunks,)),
            dma((levels,)),
            dma((levels,)),
            dma((col_n,)),
            dma,
            dma((levels,)),
            dma((levels,)),
            dma((levels,)),
            dma((levels,)),
        ],
        compiler_params=pltpu.CompilerParams(
            collective_id=0, has_side_effects=True, vmem_limit_bytes=48 * 1024 * 1024
        ),
        name="gather",
    )(matrix)
    share_rows = PANEL // row_n
    return tuple(
        pl.pallas_call(
            functools.partial(project_kernel, rows * row_n, share_rows),
            grid=(rows // PANEL,),
            out_shape=(
                jax.ShapeDtypeStruct((share_rows, cols), jnp.float32),
                jax.ShapeDtypeStruct((rows, cols), jnp.float32),
            ),
            in_specs=[
                pl.BlockSpec((PANEL, cols), lambda i: (i, 0)),
                pl.BlockSpec((PANEL, PANEL), lambda i: (i, 0)),
                pl.BlockSpec((PANEL, PANEL), lambda i: (0, 0)),
                pl.BlockSpec((PANEL, cols), lambda i: (0, 0)),
            ],
            out_specs=(
                pl.BlockSpec((share_rows, cols), lambda i: (0, 0)),
                pl.BlockSpec((PANEL, cols), lambda i: (i, 0)),
            ),
            scratch_shapes=[
                pltpu.VMEM((PANEL, cols), jnp.bfloat16),
                pltpu.VMEM((PANEL, cols), jnp.bfloat16),
            ],
            compiler_params=pltpu.CompilerParams(vmem_limit_bytes=40 * 1024 * 1024),
            name="project",
        )(matrix, panel, inverse, products)
    )


def solution(mesh):
    return jax.shard_map(
        shards,
        mesh=mesh,
        in_specs=(P("row", "col"),),
        out_specs=(P("row", "col"), P("row", "col")),
        check_vma=False,
    )
```

```python
import functools

import jax
import jax.numpy as jnp
from jax import lax
from jax.experimental import pallas as pl
from jax.experimental.pallas import tpu as pltpu
from jax.sharding import PartitionSpec as P

PANEL = 256
LANES = 128
BLOCK = 32
CHUNK = 256
TILE = 512
MESH = pl.DeviceIdType.MESH
precise = lax.Precision.HIGHEST


def multiply(left, right, dims=((1,), (0,))):
    return lax.dot_general(
        left, right, (dims, ((), ())), precision=precise, preferred_element_type=jnp.float32
    )


def quick(left, right):
    return jnp.dot(left, right, preferred_element_type=jnp.float32)


def split(value):
    high = value.astype(jnp.bfloat16)
    return high, (value - high.astype(jnp.float32)).astype(jnp.bfloat16)


def factor(work_ref, inverse_ref, between):
    row_ids = lax.broadcasted_iota(jnp.int32, (PANEL, PANEL), 0)
    col_ids = lax.broadcasted_iota(jnp.int32, (PANEL, PANEL), 1)
    work_ref[:, PANEL:] = (row_ids == col_ids).astype(jnp.float32)

    def step(k, carry):
        between(k)
        first = pl.multiple_of(k * BLOCK, BLOCK)
        rows = work_ref[pl.ds(first, BLOCK), :]
        picks_row = lax.broadcasted_iota(jnp.int32, (PANEL, 128), 0)
        picks_col = lax.broadcasted_iota(jnp.int32, (PANEL, 128), 1)
        picks = ((picks_row == picks_col + first) & (picks_col < BLOCK)).astype(jnp.float32)
        left = multiply(rows[:, :PANEL], picks)
        row = lax.broadcasted_iota(jnp.int32, (BLOCK, 128), 0)
        col = lax.broadcasted_iota(jnp.int32, (BLOCK, 128), 1)
        right = (row == col).astype(jnp.float32)
        for j in range(BLOCK):
            pivot = left[j : j + 1, j : j + 1]
            inv = lax.rsqrt(pivot)
            inv = inv * (1.5 - 0.5 * pivot * inv * inv)
            left_row = left[j : j + 1, :] * inv
            right_row = right[j : j + 1, :] * inv
            column = jnp.where(row > j, left[:, j : j + 1] * inv, 0.0)
            left = left - column * left_row
            right = jnp.where(row == j, right_row, right - column * right_row)
        solved = multiply(right[:, :BLOCK], rows)
        work_ref[pl.ds(first, BLOCK), :] = solved
        change = multiply(solved[:, :PANEL], solved, ((0,), (0,)))
        below = lax.broadcasted_iota(jnp.int32, (PANEL, 2 * PANEL), 0) >= first + BLOCK
        whole = work_ref[...]
        work_ref[...] = jnp.where(below, whole - change, whole)
        return carry

    lax.fori_loop(0, PANEL // BLOCK, step, 0)
    inverse_ref[...] = work_ref[:, PANEL:]


def gather_kernel(
    row_n,
    col_n,
    matrix_ref,
    panel_ref,
    inverse_ref,
    total_ref,
    held_ref,
    products_ref,
    gram_ref,
    gram_in_ref,
    work_ref,
    sums_in_ref,
    load_sem,
    panel_sem,
    chunk_send,
    chunk_recv,
    gram_send,
    gram_recv,
    inv_send,
    inv_recv,
    sum_send,
    sum_recv,
):
    r = lax.axis_index("row")
    z = lax.axis_index("col")
    rows, cols = held_ref.shape
    pieces = PANEL // LANES
    blocks = rows // CHUNK
    chunks = pieces * blocks
    levels = row_n.bit_length() - 1
    stages = 2 * levels

    parity = lax.rem(r, 2)
    bits = []
    for s in range(levels):
        even = 1 << s
        odd = 1 if s == 0 else 1 << (levels - s)
        bits.append(even + parity * (odd - even))
    mine = [lax.rem(lax.div(r, bit), 2) for bit in bits]
    partner = [r + bit * (1 - 2 * own) for bit, own in zip(bits, mine)]

    def span_of(i):
        return pl.ds(pl.multiple_of(i * CHUNK, CHUNK), CHUNK)

    def load(i):
        return pltpu.make_async_copy(
            matrix_ref.at[span_of(i), :], held_ref.at[span_of(i), :], load_sem.at[i]
        )

    def load_chunk(c):
        p, i = c // blocks, c % blocks
        return pltpu.make_async_copy(
            matrix_ref.at[span_of(i), pl.ds(p * LANES, LANES)],
            panel_ref.at[p, span_of(i), :],
            panel_sem.at[c],
        )

    @pl.when(z == 0)
    def _():
        for c in range(chunks):
            load_chunk(c).start()

    @pl.when(z > 0)
    def _():
        for i in range(blocks):
            load(i).start()

    barrier = pltpu.get_barrier_semaphore()
    for other in partner:
        pl.semaphore_signal(
            barrier, inc=1, device_id={"row": other, "col": z}, device_id_type=MESH
        )
    for d in range(1, col_n):
        pl.semaphore_signal(
            barrier,
            inc=1,
            device_id={"row": r, "col": lax.rem(z + d, col_n)},
            device_id_type=MESH,
        )
    pl.semaphore_wait(barrier, levels + col_n - 1)

    def send_chunk(c):
        p = lax.div(c, blocks)
        span = span_of(lax.rem(c, blocks))
        return pltpu.make_async_remote_copy(
            src_ref=panel_ref.at[p, span, :],
            dst_ref=panel_ref.at[p, span, :],
            send_sem=chunk_send.at[c],
            recv_sem=chunk_recv.at[c],
            device_id={"row": r, "col": lax.rem(z + 1, col_n)},
            device_id_type=MESH,
        )

    def add_block(c):
        p = lax.div(c, blocks)
        i = lax.rem(c, blocks)

        @pl.when(c < blocks)
        def _():
            load(i).wait()

        high, low = split(panel_ref[p, span_of(i), :].T)
        both = jnp.concatenate([high, low], axis=0)
        for t in range(0, cols, TILE):
            m_high, m_low = split(held_ref[span_of(i), pl.ds(t, TILE)])
            with_high = quick(both, m_high)
            products_ref[p, :, pl.ds(t, TILE)] += (
                with_high[:LANES] + with_high[LANES:] + quick(high, m_low)
            )

    def send_inverse(d):
        return pltpu.make_async_remote_copy(
            src_ref=inverse_ref,
            dst_ref=inverse_ref,
            send_sem=inv_send.at[d - 1],
            recv_sem=inv_recv,
            device_id={"row": r, "col": lax.rem(z + d, col_n)},
            device_id_type=MESH,
        )

    keeps, gives, sizes, offsets = [], [], [], []
    low_row, size, offset = 0, LANES, 0
    for s in range(levels):
        size //= 2
        keeps.append(pl.multiple_of(low_row + mine[s] * size, size))
        gives.append(pl.multiple_of(low_row + (1 - mine[s]) * size, size))
        sizes.append(size)
        offsets.append(offset)
        low_row = keeps[-1]
        offset += size

    def stage(p, s):
        level = s if s < levels else stages - 1 - s
        size = sizes[level]
        if s < levels:
            src = products_ref.at[p, pl.ds(gives[level], size), :]
            dst = sums_in_ref.at[p, pl.ds(offsets[level], size), :]
        else:
            src = dst = total_ref.at[p, pl.ds(keeps[level], size), :]
        return pltpu.make_async_remote_copy(
            src_ref=src,
            dst_ref=dst,
            send_sem=sum_send.at[p, s],
            recv_sem=sum_recv.at[p, s],
            device_id={"row": partner[level], "col": z},
            device_id_type=MESH,
        )

    def advance(p, s):
        if s > 0:
            stage(p, s - 1).wait()
            if s <= levels:
                span = pl.ds(keeps[s - 1], sizes[s - 1])
                arrived = pl.ds(offsets[s - 1], sizes[s - 1])
                summed_ref = total_ref if s == levels else products_ref
                summed_ref[p, span, :] = products_ref[p, span, :] + sums_in_ref[p, arrived, :]
        if s < stages:
            stage(p, s).start()

    @pl.when(z == 0)
    def _():
        for c in range(chunks):
            load_chunk(c).wait()
            send_chunk(c).start()
        for i in range(blocks):
            load(i).start()
        products_ref[...] = jnp.zeros_like(products_ref)
        gram_ref[...] = jnp.zeros_like(gram_ref)

        def gram_block(i, carry):
            part = jnp.concatenate([panel_ref[p, span_of(i), :] for p in range(pieces)], axis=1)
            gram_ref[...] += multiply(part, part, ((0,), (0,)))
            return carry

        lax.fori_loop(0, blocks, gram_block, 0)

        def filler(c, carry):
            add_block(c)
            return carry

        for s in range(levels):
            copy = pltpu.make_async_remote_copy(
                src_ref=gram_ref,
                dst_ref=gram_in_ref.at[s],
                send_sem=gram_send.at[s],
                recv_sem=gram_recv.at[s],
                device_id={"row": partner[s], "col": z},
                device_id_type=MESH,
            )
            copy.start()
            lax.fori_loop(chunks * s // levels, chunks * (s + 1) // levels, filler, 0)
            copy.wait()
            gram_ref[...] += gram_in_ref[s]
        work_ref[:, :PANEL] = gram_ref[...]
        steps = PANEL // BLOCK
        inside = min(steps, stages + 1)

        def between(k):
            for s in range(inside):

                @pl.when(k == s)
                def _():
                    for p in range(pieces):
                        advance(p, s)

        factor(work_ref, inverse_ref, between)
        for d in range(1, col_n):
            send_inverse(d).start()
        for s in range(inside, stages + 1):
            for p in range(pieces):
                advance(p, s)
        for d in range(1, col_n):
            send_inverse(d).wait_send()

    @pl.when(z > 0)
    def _():
        products_ref[...] = jnp.zeros_like(products_ref)
        inside = min(blocks, stages + 1)

        def slot(c, carry):
            copy = send_chunk(c)
            copy.wait_recv()

            @pl.when(z < col_n - 1)
            def _():
                copy.start()

            for p in range(pieces - 1):
                for s in range(inside):

                    @pl.when(c == (p + 1) * blocks + s)
                    def _():
                        advance(p, s)

            add_block(c)
            return carry

        lax.fori_loop(0, chunks, slot, 0)
        for p in range(pieces - 1):
            for s in range(inside, stages + 1):
                advance(p, s)
        for s in range(stages + 1):
            advance(pieces - 1, s)
        send_inverse(1).wait_recv()

    def drain(c, carry):
        @pl.when(z < col_n - 1)
        def _():
            send_chunk(c).wait_send()

        return carry

    lax.fori_loop(0, chunks, drain, 0)


def project_kernel(
    total_rows, share_rows, matrix_ref, panel_ref, inverse_ref, products_ref,
    share_ref, reduced_ref, high_ref, low_ref,
):
    r = lax.axis_index("row")
    z = lax.axis_index("col")
    cols = matrix_ref.shape[1]
    pieces = PANEL // LANES

    @pl.when(pl.program_id(0) == 0)
    def _():
        mine = pl.ds(pl.multiple_of(r * share_rows, share_rows), share_rows)
        for t in range(0, cols, TILE):
            tile = pl.ds(t, TILE)
            products = jnp.concatenate([products_ref[p, :, tile] for p in range(pieces)], axis=0)
            upper = multiply(inverse_ref[...], products)
            high_ref[:, tile], low_ref[:, tile] = split(upper)
            share_ref[:, tile] = multiply(inverse_ref[mine, :], products)

    rows = pl.ds(pl.multiple_of(pl.program_id(0) * PANEL, PANEL), PANEL)
    panel = jnp.concatenate([panel_ref[p, rows, :] for p in range(pieces)], axis=1)
    basis = multiply(panel, inverse_ref[...], ((1,), (1,)))
    high, low = split(basis)
    both = jnp.concatenate([high, low], axis=0)
    for t in range(0, cols, TILE):
        tile = pl.ds(t, TILE)
        with_high = quick(both, high_ref[:, tile])
        reduced_ref[:, tile] = matrix_ref[rows, tile] - (
            with_high[:PANEL] + with_high[PANEL:] + quick(high, low_ref[:, tile])
        )

    @pl.when(z == 0)
    def _():
        reduced_ref[:, :PANEL] = basis * (total_rows**0.5)


def shards(matrix):
    row_n = lax.axis_size("row")
    col_n = lax.axis_size("col")
    rows, cols = matrix.shape
    levels = row_n.bit_length() - 1
    pieces = PANEL // LANES
    blocks = rows // CHUNK
    chunks = pieces * blocks
    dma = pltpu.SemaphoreType.DMA
    vmem = pl.BlockSpec(memory_space=pltpu.VMEM)
    panel, inverse, products, held = pl.pallas_call(
        functools.partial(gather_kernel, row_n, col_n),
        out_shape=(
            jax.ShapeDtypeStruct((pieces, rows, LANES), jnp.float32),
            jax.ShapeDtypeStruct((PANEL, PANEL), jnp.float32),
            jax.ShapeDtypeStruct((pieces, LANES, cols), jnp.float32),
            jax.ShapeDtypeStruct((rows, cols), jnp.float32),
        ),
        in_specs=[pl.BlockSpec(memory_space=pl.ANY)],
        out_specs=(vmem, vmem, vmem, vmem),
        scratch_shapes=[
            pltpu.VMEM((pieces, LANES, cols), jnp.float32),
            pltpu.VMEM((PANEL, PANEL), jnp.float32),
            pltpu.VMEM((levels, PANEL, PANEL), jnp.float32),
            pltpu.VMEM((PANEL, 2 * PANEL), jnp.float32),
            pltpu.VMEM((pieces, LANES, cols), jnp.float32),
            dma((blocks,)),
            dma((chunks,)),
            dma((chunks,)),
            dma((chunks,)),
            dma((levels,)),
            dma((levels,)),
            dma((col_n,)),
            dma,
            dma((pieces, 2 * levels)),
            dma((pieces, 2 * levels)),
        ],
        compiler_params=pltpu.CompilerParams(
            collective_id=0, has_side_effects=True, vmem_limit_bytes=32 * 1024 * 1024
        ),
        name="gather",
    )(matrix)
    share_rows = PANEL // row_n
    return tuple(
        pl.pallas_call(
            functools.partial(project_kernel, rows * row_n, share_rows),
            grid=(rows // PANEL,),
            out_shape=(
                jax.ShapeDtypeStruct((share_rows, cols), jnp.float32),
                jax.ShapeDtypeStruct((rows, cols), jnp.float32),
            ),
            in_specs=[vmem, vmem, vmem, vmem],
            out_specs=(
                pl.BlockSpec((share_rows, cols), lambda i: (0, 0)),
                pl.BlockSpec((PANEL, cols), lambda i: (i, 0)),
            ),
            scratch_shapes=[
                pltpu.VMEM((PANEL, cols), jnp.bfloat16),
                pltpu.VMEM((PANEL, cols), jnp.bfloat16),
            ],
            compiler_params=pltpu.CompilerParams(vmem_limit_bytes=24 * 1024 * 1024),
            name="project",
        )(held, panel, inverse, products)
    )


def solution(mesh):
    return jax.shard_map(
        shards,
        mesh=mesh,
        in_specs=(P("row", "col"),),
        out_specs=(P("row", "col"), P("row", "col")),
        check_vma=False,
    )
```

```python
import functools

import jax
import jax.numpy as jnp
from jax import lax
from jax.experimental import pallas as pl
from jax.experimental.pallas import tpu as pltpu
from jax.sharding import PartitionSpec as P

PANEL = 256
LANES = 128
BLOCK = 32
CHUNK = 256
SENT = 128
TILE = 512
MESH = pl.DeviceIdType.MESH
precise = lax.Precision.HIGHEST


def multiply(left, right, dims=((1,), (0,))):
    return lax.dot_general(
        left, right, (dims, ((), ())), precision=precise, preferred_element_type=jnp.float32
    )


def quick(left, right):
    return jnp.dot(left, right, preferred_element_type=jnp.float32)


def split(value):
    high = value.astype(jnp.bfloat16)
    return high, (value - high.astype(jnp.float32)).astype(jnp.bfloat16)


def factor(work_ref, inverse_ref, between):
    row_ids = lax.broadcasted_iota(jnp.int32, (PANEL, PANEL), 0)
    col_ids = lax.broadcasted_iota(jnp.int32, (PANEL, PANEL), 1)
    work_ref[:, PANEL:] = (row_ids == col_ids).astype(jnp.float32)

    def step(k, carry):
        between(k)
        first = pl.multiple_of(k * BLOCK, BLOCK)
        rows = work_ref[pl.ds(first, BLOCK), :]
        picks_row = lax.broadcasted_iota(jnp.int32, (PANEL, 128), 0)
        picks_col = lax.broadcasted_iota(jnp.int32, (PANEL, 128), 1)
        picks = ((picks_row == picks_col + first) & (picks_col < BLOCK)).astype(jnp.float32)
        left = multiply(rows[:, :PANEL], picks)
        row = lax.broadcasted_iota(jnp.int32, (BLOCK, 128), 0)
        col = lax.broadcasted_iota(jnp.int32, (BLOCK, 128), 1)
        right = (row == col).astype(jnp.float32)
        for j in range(BLOCK):
            pivot = left[j : j + 1, j : j + 1]
            inv = lax.rsqrt(pivot)
            inv = inv * (1.5 - 0.5 * pivot * inv * inv)
            left_row = left[j : j + 1, :] * inv
            right_row = right[j : j + 1, :] * inv
            column = jnp.where(row > j, left[:, j : j + 1] * inv, 0.0)
            left = left - column * left_row
            right = jnp.where(row == j, right_row, right - column * right_row)
        solved = multiply(right[:, :BLOCK], rows)
        work_ref[pl.ds(first, BLOCK), :] = solved
        change = multiply(solved[:, :PANEL], solved, ((0,), (0,)))
        below = lax.broadcasted_iota(jnp.int32, (PANEL, 2 * PANEL), 0) >= first + BLOCK
        whole = work_ref[...]
        work_ref[...] = jnp.where(below, whole - change, whole)
        return carry

    lax.fori_loop(0, PANEL // BLOCK, step, 0)
    inverse_ref[...] = work_ref[:, PANEL:]


def gather_kernel(
    row_n,
    col_n,
    matrix_ref,
    panel_ref,
    inverse_ref,
    total_ref,
    held_ref,
    products_ref,
    gram_ref,
    gram_in_ref,
    work_ref,
    sums_in_ref,
    load_sem,
    panel_sem,
    chunk_send,
    chunk_recv,
    gram_send,
    gram_recv,
    inv_send,
    inv_recv,
    sum_send,
    sum_recv,
):
    r = lax.axis_index("row")
    z = lax.axis_index("col")
    rows, cols = held_ref.shape
    pieces = PANEL // LANES
    blocks = rows // CHUNK
    chunks = pieces * blocks
    levels = row_n.bit_length() - 1
    stages = 2 * levels

    parity = lax.rem(r, 2)
    bits = []
    for s in range(levels):
        even = 1 << s
        odd = 1 if s == 0 else 1 << (levels - s)
        bits.append(even + parity * (odd - even))
    mine = [lax.rem(lax.div(r, bit), 2) for bit in bits]
    partner = [r + bit * (1 - 2 * own) for bit, own in zip(bits, mine)]

    def span_of(i):
        return pl.ds(pl.multiple_of(i * CHUNK, CHUNK), CHUNK)

    def load(i):
        return pltpu.make_async_copy(
            matrix_ref.at[span_of(i), :], held_ref.at[span_of(i), :], load_sem.at[i]
        )

    def load_chunk(c):
        p, i = c // blocks, c % blocks
        return pltpu.make_async_copy(
            matrix_ref.at[span_of(i), pl.ds(p * LANES, LANES)],
            panel_ref.at[p, span_of(i), :],
            panel_sem.at[c],
        )

    @pl.when(z == 0)
    def _():
        for c in range(chunks):
            load_chunk(c).start()

    @pl.when(z > 0)
    def _():
        for i in range(blocks):
            load(i).start()

    barrier = pltpu.get_barrier_semaphore()
    for other in partner:
        pl.semaphore_signal(
            barrier, inc=1, device_id={"row": other, "col": z}, device_id_type=MESH
        )
    for d in range(1, col_n):
        pl.semaphore_signal(
            barrier,
            inc=1,
            device_id={"row": r, "col": lax.rem(z + d, col_n)},
            device_id_type=MESH,
        )
    pl.semaphore_wait(barrier, levels + col_n - 1)

    def send_chunk(c):
        per_piece = rows // SENT
        p = lax.div(c, per_piece)
        span = pl.ds(pl.multiple_of(lax.rem(c, per_piece) * SENT, SENT), SENT)
        return pltpu.make_async_remote_copy(
            src_ref=panel_ref.at[p, span, :],
            dst_ref=panel_ref.at[p, span, :],
            send_sem=chunk_send.at[c],
            recv_sem=chunk_recv.at[c],
            device_id={"row": r, "col": lax.rem(z + 1, col_n)},
            device_id_type=MESH,
        )

    def add_block(c):
        p = lax.div(c, blocks)
        i = lax.rem(c, blocks)

        @pl.when(c < blocks)
        def _():
            load(i).wait()

        high, low = split(panel_ref[p, span_of(i), :].T)
        both = jnp.concatenate([high, low], axis=0)
        for t in range(0, cols, TILE):
            m_high, m_low = split(held_ref[span_of(i), pl.ds(t, TILE)])
            with_high = quick(both, m_high)
            products_ref[p, :, pl.ds(t, TILE)] += (
                with_high[:LANES] + with_high[LANES:] + quick(high, m_low)
            )

    def send_inverse(d):
        return pltpu.make_async_remote_copy(
            src_ref=inverse_ref,
            dst_ref=inverse_ref,
            send_sem=inv_send.at[d - 1],
            recv_sem=inv_recv,
            device_id={"row": r, "col": lax.rem(z + d, col_n)},
            device_id_type=MESH,
        )

    keeps, gives, sizes, offsets = [], [], [], []
    low_row, size, offset = 0, LANES, 0
    for s in range(levels):
        size //= 2
        keeps.append(pl.multiple_of(low_row + mine[s] * size, size))
        gives.append(pl.multiple_of(low_row + (1 - mine[s]) * size, size))
        sizes.append(size)
        offsets.append(offset)
        low_row = keeps[-1]
        offset += size

    def stage(p, s):
        level = s if s < levels else stages - 1 - s
        size = sizes[level]
        if s < levels:
            src = products_ref.at[p, pl.ds(gives[level], size), :]
            dst = sums_in_ref.at[p, pl.ds(offsets[level], size), :]
        else:
            src = dst = total_ref.at[p, pl.ds(keeps[level], size), :]
        return pltpu.make_async_remote_copy(
            src_ref=src,
            dst_ref=dst,
            send_sem=sum_send.at[p, s],
            recv_sem=sum_recv.at[p, s],
            device_id={"row": partner[level], "col": z},
            device_id_type=MESH,
        )

    def advance(p, s):
        if s > 0:
            stage(p, s - 1).wait()
            if s <= levels:
                span = pl.ds(keeps[s - 1], sizes[s - 1])
                arrived = pl.ds(offsets[s - 1], sizes[s - 1])
                summed_ref = total_ref if s == levels else products_ref
                summed_ref[p, span, :] = products_ref[p, span, :] + sums_in_ref[p, arrived, :]
        if s < stages:
            stage(p, s).start()

    @pl.when(z == 0)
    def _():
        for c in range(chunks):
            load_chunk(c).wait()
            for h in range(CHUNK // SENT):
                send_chunk(c * (CHUNK // SENT) + h).start()
        for i in range(blocks):
            load(i).start()
        products_ref[...] = jnp.zeros_like(products_ref)
        gram_ref[...] = jnp.zeros_like(gram_ref)

        def gram_block(i, carry):
            part = jnp.concatenate([panel_ref[p, span_of(i), :] for p in range(pieces)], axis=1)
            gram_ref[...] += multiply(part, part, ((0,), (0,)))
            return carry

        lax.fori_loop(0, blocks, gram_block, 0)

        early = (pieces - 1) * blocks

        def filler(c, carry):
            add_block(c)
            return carry

        for s in range(levels):
            copy = pltpu.make_async_remote_copy(
                src_ref=gram_ref,
                dst_ref=gram_in_ref.at[s],
                send_sem=gram_send.at[s],
                recv_sem=gram_recv.at[s],
                device_id={"row": partner[s], "col": z},
                device_id_type=MESH,
            )
            copy.start()
            lax.fori_loop(early * s // levels, early * (s + 1) // levels, filler, 0)
            copy.wait()
            gram_ref[...] += gram_in_ref[s]
        work_ref[:, :PANEL] = gram_ref[...]
        steps = PANEL // BLOCK
        inside = min(steps, stages + 1)

        def between(k):
            for s in range(inside):

                @pl.when(k == s)
                def _():
                    for p in range(pieces - 1):
                        advance(p, s)

        factor(work_ref, inverse_ref, between)
        for d in range(1, col_n):
            send_inverse(d).start()
        for s in range(inside, stages + 1):
            for p in range(pieces - 1):
                advance(p, s)
        lax.fori_loop(early, chunks, filler, 0)

    @pl.when(z > 0)
    def _():
        products_ref[...] = jnp.zeros_like(products_ref)
        inside = min(blocks, stages + 1)

        def slot(c, carry):
            for h in range(CHUNK // SENT):
                copy = send_chunk(c * (CHUNK // SENT) + h)
                copy.wait_recv()
                pl.when(z < col_n - 1)(copy.start)

            for p in range(pieces - 1):
                for s in range(inside):

                    @pl.when(c == (p + 1) * blocks + s)
                    def _():
                        advance(p, s)

            add_block(c)
            return carry

        lax.fori_loop(0, chunks, slot, 0)
        for p in range(pieces - 1):
            for s in range(inside, stages + 1):
                advance(p, s)

    def drain(c, carry):
        pl.when(z < col_n - 1)(send_chunk(c).wait_send)
        return carry

    def form_basis(i, carry):
        block = jnp.concatenate([panel_ref[p, span_of(i), :] for p in range(pieces)], axis=1)
        basis = multiply(block, inverse_ref[...], ((1,), (1,)))
        for p in range(pieces):
            panel_ref[p, span_of(i), :] = basis[:, p * LANES : (p + 1) * LANES]
        return carry

    for s in range(stages + 1):
        advance(pieces - 1, s)
        if s == levels:
            lax.fori_loop(0, chunks * CHUNK // SENT, drain, 0)
            pl.when(z > 0)(send_inverse(1).wait_recv)
        if levels <= s < stages:
            done = s - levels
            lax.fori_loop(
                blocks * done // levels, blocks * (done + 1) // levels, form_basis, 0
            )

    @pl.when(z == 0)
    def _():
        for d in range(1, col_n):
            send_inverse(d).wait_send()


def project_kernel(
    total_rows, share_rows, matrix_ref, panel_ref, inverse_ref, products_ref,
    share_ref, reduced_ref, high_ref, low_ref,
):
    r = lax.axis_index("row")
    z = lax.axis_index("col")
    cols = matrix_ref.shape[1]
    pieces = PANEL // LANES

    @pl.when(pl.program_id(0) == 0)
    def _():
        mine = pl.ds(pl.multiple_of(r * share_rows, share_rows), share_rows)
        for t in range(0, cols, TILE):
            tile = pl.ds(t, TILE)
            products = jnp.concatenate([products_ref[p, :, tile] for p in range(pieces)], axis=0)
            upper = multiply(inverse_ref[...], products)
            high_ref[:, tile], low_ref[:, tile] = split(upper)
            share_ref[:, tile] = multiply(inverse_ref[mine, :], products)

    rows = pl.ds(pl.multiple_of(pl.program_id(0) * PANEL, PANEL), PANEL)
    basis = jnp.concatenate([panel_ref[p, rows, :] for p in range(pieces)], axis=1)
    high, low = split(basis)
    both = jnp.concatenate([high, low], axis=0)
    for t in range(0, cols, TILE):
        tile = pl.ds(t, TILE)
        with_high = quick(both, high_ref[:, tile])
        reduced_ref[:, tile] = matrix_ref[rows, tile] - (
            with_high[:PANEL] + with_high[PANEL:] + quick(high, low_ref[:, tile])
        )

    @pl.when(z == 0)
    def _():
        reduced_ref[:, :PANEL] = basis * (total_rows**0.5)


def shards(matrix):
    row_n = lax.axis_size("row")
    col_n = lax.axis_size("col")
    rows, cols = matrix.shape
    levels = row_n.bit_length() - 1
    pieces = PANEL // LANES
    blocks = rows // CHUNK
    chunks = pieces * blocks
    dma = pltpu.SemaphoreType.DMA
    vmem = pl.BlockSpec(memory_space=pltpu.VMEM)
    panel, inverse, products, held = pl.pallas_call(
        functools.partial(gather_kernel, row_n, col_n),
        out_shape=(
            jax.ShapeDtypeStruct((pieces, rows, LANES), jnp.float32),
            jax.ShapeDtypeStruct((PANEL, PANEL), jnp.float32),
            jax.ShapeDtypeStruct((pieces, LANES, cols), jnp.float32),
            jax.ShapeDtypeStruct((rows, cols), jnp.float32),
        ),
        in_specs=[pl.BlockSpec(memory_space=pl.ANY)],
        out_specs=(vmem, vmem, vmem, vmem),
        scratch_shapes=[
            pltpu.VMEM((pieces, LANES, cols), jnp.float32),
            pltpu.VMEM((PANEL, PANEL), jnp.float32),
            pltpu.VMEM((levels, PANEL, PANEL), jnp.float32),
            pltpu.VMEM((PANEL, 2 * PANEL), jnp.float32),
            pltpu.VMEM((pieces, LANES, cols), jnp.float32),
            dma((blocks,)),
            dma((chunks,)),
            dma((chunks * CHUNK // SENT,)),
            dma((chunks * CHUNK // SENT,)),
            dma((levels,)),
            dma((levels,)),
            dma((col_n,)),
            dma,
            dma((pieces, 2 * levels)),
            dma((pieces, 2 * levels)),
        ],
        compiler_params=pltpu.CompilerParams(
            collective_id=0, has_side_effects=True, vmem_limit_bytes=32 * 1024 * 1024
        ),
        name="gather",
    )(matrix)
    share_rows = PANEL // row_n
    return tuple(
        pl.pallas_call(
            functools.partial(project_kernel, rows * row_n, share_rows),
            grid=(rows // PANEL,),
            out_shape=(
                jax.ShapeDtypeStruct((share_rows, cols), jnp.float32),
                jax.ShapeDtypeStruct((rows, cols), jnp.float32),
            ),
            in_specs=[vmem, vmem, vmem, vmem],
            out_specs=(
                pl.BlockSpec((share_rows, cols), lambda i: (0, 0)),
                pl.BlockSpec((PANEL, cols), lambda i: (i, 0)),
            ),
            scratch_shapes=[
                pltpu.VMEM((PANEL, cols), jnp.bfloat16),
                pltpu.VMEM((PANEL, cols), jnp.bfloat16),
            ],
            compiler_params=pltpu.CompilerParams(vmem_limit_bytes=24 * 1024 * 1024),
            name="project",
        )(held, panel, inverse, products)
    )


def solution(mesh):
    return jax.shard_map(
        shards,
        mesh=mesh,
        in_specs=(P("row", "col"),),
        out_specs=(P("row", "col"), P("row", "col")),
        check_vma=False,
    )
```
